16 devices in a mesh: dp: 2 (over y, z), sp: 8 (over x, core).
Axes of the slice: x: 4, y: 2, z: 1, core: 2. Of those that a mesh axis runs over, the one named last changes fastest.
The devices are a block of a 4x4x4 slice.
Arguments:
- x: bfloat16 [4096, 12288], P(('dp', 'sp')), parts along dimension 0
- gain: bfloat16 [12288], replicated
- wq: bfloat16 [12288, 12288], replicated
- wk: bfloat16 [12288, 1024], replicated
- wv: bfloat16 [12288, 1024], replicated
- wo: bfloat16 [12288, 12288], replicated
Outputs:
- output: bfloat16 [4096, 12288], P(('dp', 'sp')), parts along dimension 0
There are 2 independent parts. The reference program is written for one: setup_inputs(seed, part) draws one part's arguments, and reference() takes and returns one part's arrays. A program takes and returns all parts, laid end to end along the dimension named above; an argument that names none is the same for every part.
All inputs are finite; a program needn't handle non-finite values.
Results may differ from the reference program's by a relative error of at most 0.012.
Values are sent between devices in bfloat16 or wider.
A program may use at most 1.5 GiB of HBM per device.

```python
import jax
import jax.numpy as jnp
from jax import lax

ROWS = 2048
D = 12288
HEADS = 96
KV_HEADS = 8
HEAD = 128
THETA = 10000


def setup_inputs(seed: int = 0, part: int = 0) -> dict:
    kx, kn, kq, kk, kv, ko = jax.random.split(jax.random.key(seed), 6)

    def weights(key, rows, columns):
        return jax.random.normal(key, (rows, columns), jnp.float32) * rows**-0.5

    drawn = {
        "x": jax.random.normal(jax.random.fold_in(kx, part), (ROWS, D), jnp.float32),
        "gain": 1 + 0.1 * jax.random.normal(kn, (D,), jnp.float32),
        "wq": 2 * weights(kq, D, HEADS * HEAD),
        "wk": 2 * weights(kk, D, KV_HEADS * HEAD),
        "wv": 4 * weights(kv, D, KV_HEADS * HEAD),
        "wo": weights(ko, HEADS * HEAD, D),
    }
    return {k: v.astype(jnp.bfloat16) for k, v in drawn.items()}


def normed(x, gain):
    wide = x.astype(jnp.float32)
    scale = lax.rsqrt(jnp.mean(wide * wide, -1, keepdims=True) + 1e-6)
    return (wide * scale * gain.astype(jnp.float32)).astype(jnp.bfloat16)


def turned(t, place, theta):
    half = t.shape[-1] // 2
    angle = place.astype(jnp.float32)[:, None] * theta ** (-jnp.arange(half, dtype=jnp.float32) / half)
    cos, sin = jnp.cos(angle)[:, None], jnp.sin(angle)[:, None]
    a, b = t[..., :half].astype(jnp.float32), t[..., half:].astype(jnp.float32)
    return jnp.concatenate([a * cos - b * sin, b * cos + a * sin], -1).astype(jnp.bfloat16)


def matmul(a, w):
    return jnp.dot(a, w, preferred_element_type=jnp.float32).astype(jnp.bfloat16)


def einsum(form, a, b):
    return jnp.einsum(form, a.astype(jnp.float32), b.astype(jnp.float32))


def attention(q, k, v):
    scores = einsum("tgsd,ugd->gstu", q, k) * q.shape[-1] ** -0.5
    token = jnp.arange(q.shape[0])
    scores = jnp.where(token[:, None] >= token, scores, -jnp.inf)
    weights = jax.nn.softmax(scores, -1).astype(jnp.bfloat16)
    return einsum("gstu,ugd->tgsd", weights, v).astype(jnp.bfloat16)


def reference(x, gain, wq, wk, wv, wo):
    a, place = normed(x, gain), jnp.arange(ROWS)
    q = turned(matmul(a, wq).reshape(ROWS, HEADS, HEAD), place, THETA).reshape(ROWS, KV_HEADS, -1, HEAD)
    k = turned(matmul(a, wk).reshape(ROWS, KV_HEADS, HEAD), place, THETA)
    v = matmul(a, wv).reshape(ROWS, KV_HEADS, HEAD)
    seen = attention(q, k, v).reshape(ROWS, HEADS * HEAD)
    return (x.astype(jnp.float32) + jnp.dot(seen, wo, preferred_element_type=jnp.float32)).astype(jnp.bfloat16)
```

```python
import functools

import jax
import jax.numpy as jnp
from jax import lax
from jax.experimental import pallas as pl
from jax.experimental.pallas import tpu as pltpu
from jax.sharding import PartitionSpec as P

HEAD = 128
THETA = 10000
NEG = -1e30
HIDDEN = 2 * NEG
LOG2E = 1.4426950408889634
VMEM = 64 * 2**20 - 2**16
MESH = pl.DeviceIdType.MESH

TILE = 512
DEPTH = 3
OUT_TILE = 2048
OUT_DEPTH = 3
STRIP = 512


def _dot(a, b, ca=1, cb=0):
    return lax.dot_general(a, b, (((ca,), (cb,)), ((), ())), preferred_element_type=jnp.float32)


def _offset(s, n):
    far = n // 2 - 1
    last = s // (2 * far)
    d = (s % far + 1) * (1 - last)
    e = (s // far) * (1 - last) + (n - 1 - s) * last
    return d, e


def _target(me, s, n):
    d, e = _offset(s, n)
    return ((me // 2 + d) % (n // 2)) * 2 + (me % 2 + e) % 2


def _source(me, s, n):
    d, e = _offset(s, n)
    return ((me // 2 + n // 2 - d) % (n // 2)) * 2 + (me % 2 + e) % 2


def _greet(me, n):
    barrier = pltpu.get_barrier_semaphore()
    for i in range(1, n):
        pl.semaphore_signal(barrier, inc=1, device_id={"sp": (me + i) % n}, device_id_type=MESH)
    return barrier


def _project(n, heads, x_hbm, gain_ref, rot_ref, wq_hbm, wk_hbm, wv_hbm, out_hbm, a_s, w_s, stage_s, x_sem, w_sem, own_sem, send_sem, recv_sem):
    me = lax.axis_index("sp")
    tile = w_s.shape[2]
    per = heads * HEAD // tile
    kt = wk_hbm.shape[1] // tile
    total = 2 * kt + n * per
    wide = tile // HEAD

    get_x = pltpu.make_async_copy(x_hbm, a_s, x_sem)
    get_x.start()

    def fetch(t):
        slot = t % DEPTH

        def start(ref, column):
            pltpu.make_async_copy(ref.at[:, pl.ds(pl.multiple_of(column, tile), tile)], w_s.at[slot], w_sem.at[slot]).start()

        @pl.when(t < kt)
        def _():
            start(wk_hbm, t * tile)

        @pl.when((t >= kt) & (t < 2 * kt))
        def _():
            start(wv_hbm, (t - kt) * tile)

        @pl.when((t >= 2 * kt) & (t < total))
        def _():
            j = t - 2 * kt
            start(wq_hbm, (_target(me, j // per, n) * per + j % per) * tile)

    for t in range(DEPTH - 1):
        fetch(jnp.int32(t))
    barrier = _greet(me, n)

    get_x.wait()

    def norm(i, _):
        rows = pl.ds(pl.multiple_of(i * 16, 16), 16)
        w = a_s[rows, :].astype(jnp.float32)
        scale = lax.rsqrt(jnp.mean(w * w, -1, keepdims=True) + 1e-6)
        a_s[rows, :] = (w * scale * gain_ref[...].astype(jnp.float32)).astype(jnp.bfloat16)

    lax.fori_loop(0, a_s.shape[0] // 16, norm, None)
    pl.semaphore_wait(barrier, n - 1)

    def send(kind, to):
        part = pl.ds(0, 2) if kind == 0 else pl.ds(2, heads)
        return pltpu.make_async_remote_copy(
            src_ref=stage_s.at[to, part], dst_ref=out_hbm.at[me, part], send_sem=send_sem.at[kind, to], recv_sem=recv_sem.at[kind, me],
            device_id={"sp": to}, device_id_type=MESH)

    def arrived(kind, source):
        part = pl.ds(0, 2) if kind == 0 else pl.ds(2, heads)
        return pltpu.make_async_remote_copy(
            src_ref=stage_s.at[source, part], dst_ref=out_hbm.at[source, part], send_sem=send_sem.at[kind, source],
            recv_sem=recv_sem.at[kind, source], device_id={"sp": source}, device_id_type=MESH)

    def step(t, _):
        slot = t % DEPTH
        pltpu.make_async_copy(wq_hbm.at[:, pl.ds(0, tile)], w_s.at[slot], w_sem.at[slot]).wait()
        fetch(t + DEPTH - 1)
        made = _dot(a_s[...], w_s[slot]).astype(jnp.bfloat16).astype(jnp.float32)

        def put(i, to, place, turn):
            got = made[:, i * HEAD : (i + 1) * HEAD]
            if turn:
                got = got * rot_ref[0] + pltpu.roll(got, HEAD // 2, 1) * rot_ref[1]
            stage_s[to, place] = got.astype(jnp.bfloat16)

        @pl.when(t < kt)
        def _():
            for i in range(wide):
                put(i, t * wide + i, 0, True)

        @pl.when((t >= kt) & (t < 2 * kt))
        def _():
            for i in range(wide):
                put(i, (t - kt) * wide + i, 1, False)

        @pl.when(t == 2 * kt - 1)
        def _():
            for s in range(n - 1):
                send(0, _target(me, s, n)).start()

        @pl.when(t >= 2 * kt)
        def _():
            j = t - 2 * kt
            to = _target(me, j // per, n)
            for i in range(wide):
                put(i, to, 2 + (j % per) * wide + i, True)

            @pl.when((j % per == per - 1) & (j // per < n - 1))
            def _():
                send(1, to).start()

    lax.fori_loop(0, total, step, None)
    keep = pltpu.make_async_copy(stage_s.at[me], out_hbm.at[me], own_sem)
    keep.start()
    for kind in range(2):
        for s in range(n - 1):
            send(kind, _target(me, s, n)).wait_send()
    for kind in range(2):
        for s in range(n - 1):
            arrived(kind, _source(me, s, n)).wait_recv()
    keep.wait()


def project(x, gain, rot, wq, wk, wv, n):
    own, d = x.shape
    heads = wq.shape[1] // HEAD // n
    any_ = pl.BlockSpec(memory_space=pltpu.HBM)
    vmem = pl.BlockSpec(memory_space=pltpu.VMEM)
    return pl.pallas_call(
        functools.partial(_project, n, heads),
        out_shape=jax.ShapeDtypeStruct((n, 2 + heads, own, HEAD), jnp.bfloat16),
        in_specs=[any_, vmem, vmem, any_, any_, any_],
        out_specs=any_,
        scratch_shapes=[
            pltpu.VMEM((own, d), jnp.bfloat16),
            pltpu.VMEM((DEPTH, d, TILE), jnp.bfloat16),
            pltpu.VMEM((n, 2 + heads, own, HEAD), jnp.bfloat16),
            pltpu.SemaphoreType.DMA,
            pltpu.SemaphoreType.DMA((DEPTH,)),
            pltpu.SemaphoreType.DMA,
            pltpu.SemaphoreType.DMA((2, n)),
            pltpu.SemaphoreType.DMA((2, n)),
        ],
        compiler_params=pltpu.CompilerParams(collective_id=0, has_side_effects=True, vmem_limit_bytes=VMEM),
        name="project",
    )(x, gain[None], rot, wq, wk, wv)


def _finish(n, heads, qkv_hbm, x_hbm, wo_hbm, y_hbm, kv_s, vt_s, q_s, top_s, mix_s, gap_s, buf_s, acc_s, w_s, y_s,
            x_sem, kv_sem, q_sem, w_sem, y_sem, send_sem, recv_sem):
    me = lax.axis_index("sp")
    own = q_s.shape[2]
    width = heads * HEAD
    cols = heads * own
    tile = w_s.shape[2]
    per = wo_hbm.shape[1] // tile
    total = n * per
    e = HEAD**-0.5 * LOG2E

    get_kv = [pltpu.make_async_copy(qkv_hbm.at[:, i], kv_s.at[i], kv_sem.at[i]) for i in range(2)]

    def get_q(s):
        return pltpu.make_async_copy(qkv_hbm.at[_target(me, s, n), pl.ds(2, heads)], q_s.at[s % 2], q_sem.at[s % 2])

    get_x = [pltpu.make_async_copy(x_hbm.at[:, pl.ds(i * width, width)], buf_s.at[i], x_sem.at[i]) for i in range(n)]
    for copy in get_kv:
        copy.start()
    get_q(jnp.int32(0)).start()
    for copy in get_x:
        copy.start()

    def turn(u):
        early = 1 - jnp.minimum(u // 2, 1)
        return early * (n - 1 - u) + (1 - early) * (u - 2)

    def fetch(t):
        slot = t % OUT_DEPTH
        rows = _source(me, turn(t // per), n) * width
        return pltpu.make_async_copy(
            wo_hbm.at[pl.ds(pl.multiple_of(rows, width), width), pl.ds(pl.multiple_of(t % per * tile, tile), tile)], w_s.at[slot], w_sem.at[slot])

    for t in range(OUT_DEPTH - 1):
        fetch(jnp.int32(t)).start()
    barrier = _greet(me, n)

    for copy in get_kv:
        copy.wait()
    for j in range(n):
        vt_s[:HEAD, j * own : (j + 1) * own] = kv_s[1, j].T
    vt_s[HEAD:, :] = jnp.ones((vt_s.shape[0] - HEAD, n * own), jnp.bfloat16)
    bk2 = 2 * own
    gap_s[...] = lax.rem(lax.broadcasted_iota(jnp.int32, gap_s.shape, 1), own) - lax.broadcasted_iota(jnp.int32, gap_s.shape, 0)
    for i in range(n):
        get_x[i].wait()
        acc_s[:, i * width : (i + 1) * width] = buf_s[i].astype(jnp.float32)
    pl.semaphore_wait(barrier, n - 1)

    starts = list(range(0, cols, STRIP))

    def block(slot, first, count, level):
        bk = count * own
        k = kv_s[0, pl.ds(first, count)].reshape(bk, HEAD)
        vt = vt_s[:, pl.ds(pl.multiple_of(first * own, own), bk)]
        q = q_s.at[slot]

        def score(at):
            return _dot(k, q[at // own : (at + STRIP) // own].reshape(STRIP, HEAD), 1, 1)

        def weigh(at, s):
            here = slice(at, at + STRIP)
            if level is not None:
                s = jnp.where(gap_s[:bk, :] >= -level, s, HIDDEN)
            old = top_s[:, here]
            top = jnp.maximum(old, s.max(axis=0, keepdims=True))
            top_s[:, here] = top
            return jnp.exp2((s - top) * e).astype(jnp.bfloat16), jnp.exp2((old - top) * e)

        def mix(at, p, keep):
            here = slice(at, at + STRIP)
            mix_s[:, here] = mix_s[:, here] * keep + _dot(vt, p)

        s_next, before = score(starts[0]), None
        for i, at in enumerate(starts):
            s = s_next
            if i + 1 < len(starts):
                s_next = score(starts[i + 1])
            p, keep = weigh(at, s)
            if before is not None:
                mix(*before)
            before = (at, p, keep)
        mix(*before)

    def send(to, slot):
        return pltpu.make_async_remote_copy(
            src_ref=buf_s.at[slot], dst_ref=buf_s.at[n + me], send_sem=send_sem.at[to], recv_sem=recv_sem.at[me],
            device_id={"sp": to}, device_id_type=MESH)

    def attend(s, _):
        b = _target(me, s, n)
        slot = s % 2
        get_q(s).wait()

        @pl.when(s + 1 < n)
        def _():
            get_q(s + 1).start()

        top_s[...] = jnp.full(top_s.shape, NEG, jnp.float32)
        mix_s[...] = jnp.zeros(mix_s.shape, jnp.float32)
        lax.fori_loop(0, b // 2, lambda j, _: block(slot, 2 * j, 2, None), None)

        @pl.when(b % 2 == 0)
        def _():
            block(slot, b, 1, 0)

        @pl.when(b % 2 == 1)
        def _():
            block(slot, b - 1, 2, own)

        mine = s // (n - 1)
        to = b * (1 - mine) + (n + me) * mine
        for h in range(heads):
            here = slice(h * own, (h + 1) * own)
            buf_s[to, :, h * HEAD : (h + 1) * HEAD] = (mix_s[:HEAD, here] * (1 / mix_s[HEAD : HEAD + 1, here])).T.astype(jnp.bfloat16)

        @pl.when(s < n - 1)
        def _():
            send(b, b).start()

    lax.fori_loop(0, n, attend, None)

    def put(t):
        return pltpu.make_async_copy(y_s.at[t % 2], y_hbm.at[:, pl.ds(pl.multiple_of(t % per * tile, tile), tile)], y_sem.at[t % 2])

    def step(t, _):
        u = t // per
        slot = t % OUT_DEPTH
        src = _source(me, turn(u), n)

        @pl.when((t % per == 0) & (u > 0))
        def _():
            pltpu.make_async_remote_copy(
                src_ref=buf_s.at[src], dst_ref=buf_s.at[n + src], send_sem=send_sem.at[src], recv_sem=recv_sem.at[src],
                device_id={"sp": src}, device_id_type=MESH).wait_recv()

        fetch(t).wait()

        @pl.when(t + OUT_DEPTH - 1 < total)
        def _():
            fetch(t + OUT_DEPTH - 1).start()

        here = pl.ds(pl.multiple_of(t % per * tile, tile), tile)
        acc_s[:, here] += _dot(buf_s[n + src], w_s[slot])

        @pl.when(u == n - 1)
        def _():
            @pl.when(t % per >= 2)
            def _():
                put(t - 2).wait()

            y_s[t % 2] = acc_s[:, here].astype(jnp.bfloat16)
            put(t).start()

    lax.fori_loop(0, total, step, None)
    for t in range(total - 2, total):
        put(jnp.int32(t)).wait()
    for s in range(n - 1):
        to = _target(me, s, n)
        send(to, to).wait_send()


def finish(qkv, x, wo, n):
    own, d = x.shape
    heads = qkv.shape[1] - 2
    hbm = pl.BlockSpec(memory_space=pltpu.HBM)
    cols = heads * own
    return pl.pallas_call(
        functools.partial(_finish, n, heads),
        out_shape=jax.ShapeDtypeStruct((own, wo.shape[1]), jnp.bfloat16),
        in_specs=[hbm] * 3,
        out_specs=hbm,
        scratch_shapes=[
            pltpu.VMEM((2, n, own, HEAD), jnp.bfloat16),
            pltpu.VMEM((HEAD + 16, n * own), jnp.bfloat16),
            pltpu.VMEM((2, heads, own, HEAD), jnp.bfloat16),
            pltpu.VMEM((1, cols), jnp.float32),
            pltpu.VMEM((HEAD + 16, cols), jnp.float32),
            pltpu.VMEM((2 * own, STRIP), jnp.int32),
            pltpu.VMEM((2 * n, own, heads * HEAD), jnp.bfloat16),
            pltpu.VMEM((own, wo.shape[1]), jnp.float32),
            pltpu.VMEM((OUT_DEPTH, heads * HEAD, OUT_TILE), jnp.bfloat16),
            pltpu.VMEM((2, own, OUT_TILE), jnp.bfloat16),
            pltpu.SemaphoreType.DMA((n,)),
            pltpu.SemaphoreType.DMA((2,)),
            pltpu.SemaphoreType.DMA((2,)),
            pltpu.SemaphoreType.DMA((OUT_DEPTH,)),
            pltpu.SemaphoreType.DMA((2,)),
            pltpu.SemaphoreType.DMA((n,)),
            pltpu.SemaphoreType.DMA((n,)),
        ],
        compiler_params=pltpu.CompilerParams(collective_id=1, has_side_effects=True, vmem_limit_bytes=VMEM),
        name="finish",
    )(qkv, x, wo)


def solution(mesh):
    n = mesh.shape["sp"]

    def step(x, gain, wq, wk, wv, wo):
        own = x.shape[0]
        place = (lax.axis_index("sp") * own + jnp.arange(own)).astype(jnp.float32)
        half = HEAD // 2
        angle = place[:, None] * THETA ** (-jnp.arange(half, dtype=jnp.float32) / half)
        cos, sin = jnp.cos(angle), jnp.sin(angle)
        rot = jnp.stack([jnp.concatenate([cos, cos], -1), jnp.concatenate([-sin, sin], -1)])
        qkv = project(x, gain, rot, wq, wk, wv, n)
        return finish(qkv, x, wo, n)

    tokens, whole = P(("dp", "sp"), None), P(None, None)
    return jax.shard_map(
        step,
        mesh=mesh,
        in_specs=(tokens, P(None), whole, whole, whole, whole),
        out_specs=tokens,
        check_vma=False,
    )
```

```python
import functools

import jax
import jax.numpy as jnp
from jax import lax
from jax.experimental import pallas as pl
from jax.experimental.pallas import tpu as pltpu
from jax.sharding import PartitionSpec as P

HEAD = 128
THETA = 10000
NEG = -1e30
HIDDEN = 2 * NEG
LOG2E = 1.4426950408889634
VMEM = 64 * 2**20 - 2**16
MESH = pl.DeviceIdType.MESH

DEPTH = 3
OUT_TILE = 1024
OUT_DEPTH = 4
SLOTS = 3
LAG = 2
STRIP = 512
ROWS, CHUNK = 64, 512


def _dot(a, b, ca=1, cb=0):
    return lax.dot_general(a, b, (((ca,), (cb,)), ((), ())), preferred_element_type=jnp.float32)


def _away(s, chips):
    far = chips - 1
    last = s // (2 * far)
    return (s % far + 1) * (1 - last), s // far * (1 - last) + (s - 2 * far) * last


def _greet(me, n):
    barrier = pltpu.get_barrier_semaphore()
    for i in range(1, n):
        pl.semaphore_signal(barrier, inc=1, device_id={"sp": (me + i) % n}, device_id_type=MESH)
    return barrier


def _project(n, heads, x_hbm, gain_ref, rot_ref, wq_hbm, wk_hbm, wv_hbm, out_hbm, a_s, w_s, stage_s, raw_s,
             x_sem, w_sem, a_send, a_recv, own_sem, send_sem, recv_sem):
    me = lax.axis_index("sp")
    chip, core = me // 2, me % 2
    chips, partner = n // 2, me // 2 * 2 + 1 - me % 2
    own, d = x_hbm.shape
    tile = w_s.shape[2]
    wide = tile // HEAD
    per = heads * HEAD // tile
    both = 2 + heads
    tiles = 2 + chips * per
    total = 2 * tiles

    get_x = pltpu.make_async_copy(x_hbm, a_s.at[pl.ds(0, own)], x_sem)
    get_x.start()

    def query(t):
        j, far = jnp.maximum(t - 2, 0), chips - 1
        last = jnp.minimum(j // (per * far), 1)
        return (j % far + 1) * (1 - last), j // far * (1 - last) + (j - per * far) * last

    def fetch(t):
        slot = t % DEPTH

        def pair(ref):
            for i in range(chips):
                pltpu.make_async_copy(ref.at[:, pl.ds(pl.multiple_of((2 * i + core) * HEAD, HEAD), HEAD)],
                                      w_s.at[slot, :, pl.ds(i * HEAD, HEAD)], w_sem.at[slot]).start()

        @pl.when(t == 0)
        def _():
            pair(wk_hbm)

        @pl.when(t == 1)
        def _():
            pair(wv_hbm)

        @pl.when((t >= 2) & (t < tiles))
        def _():
            away, sub = query(t)
            column = (((chip + away) % chips * 2 + core) * per + sub) * tile
            pltpu.make_async_copy(wq_hbm.at[:, pl.ds(pl.multiple_of(column, tile), tile)], w_s.at[slot], w_sem.at[slot]).start()

    for t in range(DEPTH):
        fetch(jnp.int32(t))
    barrier = _greet(me, n)

    def norm(i):
        rows = pl.ds(pl.multiple_of(i * ROWS, ROWS), ROWS)

        def chunk(c):
            return pl.ds(pl.multiple_of(c * CHUNK, CHUNK), CHUNK)

        def square(c, total):
            w = a_s[rows, chunk(c)].astype(jnp.float32)
            w = w * w
            return total + sum(w[:, k : k + HEAD] for k in range(0, CHUNK, HEAD))

        total = lax.fori_loop(0, d // CHUNK, square, jnp.zeros((ROWS, HEAD), jnp.float32))
        scale = lax.rsqrt(total.sum(-1, keepdims=True) * (1 / d) + 1e-6)

        def apply(c, _):
            w = a_s[rows, chunk(c)].astype(jnp.float32)
            a_s[rows, chunk(c)] = (w * scale * gain_ref[:, chunk(c)].astype(jnp.float32)).astype(jnp.bfloat16)

        lax.fori_loop(0, d // CHUNK, apply, None)

    def swap(i):
        return pltpu.make_async_remote_copy(
            src_ref=a_s.at[pl.ds(i * ROWS, ROWS)], dst_ref=a_s.at[pl.ds(own + i * ROWS, ROWS)], send_sem=a_send.at[i], recv_sem=a_recv.at[i],
            device_id={"sp": partner}, device_id_type=MESH)

    get_x.wait()
    pl.semaphore_wait(barrier, n - 1)
    for i in range(own // ROWS):
        norm(i)
        swap(i).start()

    def unit(u):
        early = 1 - jnp.minimum(u // 4, 1)
        return early * (u % 2) + (1 - early) * (u // 2), early * (u // 2) + (1 - early) * (u % 2)

    def block(half):
        return chip * 2 + (core + half) % 2

    def turn(u):
        t, half = unit(u)
        away, sub = query(t)
        q = jnp.minimum(t // 2, 1)
        base = q * (((chip + away) % chips * 2 + half) * both + 2 + sub * wide) + (1 - q) * (half * both + t)
        gap = q + (1 - q) * 2 * both
        angle = q * half + (1 - q) * (half * (1 - t) + 2 * t)
        for i in range(wide):
            got = raw_s[u % 2, :, i * HEAD : (i + 1) * HEAD].astype(jnp.bfloat16).astype(jnp.float32)
            got = got * rot_ref[angle, 0] + pltpu.roll(got, HEAD // 2, 1) * rot_ref[angle, 1]
            stage_s[base + i * gap] = got.astype(jnp.bfloat16)

    def send(away, half, kind, count, first):
        to = (chip + away) % chips
        return pltpu.make_async_remote_copy(
            src_ref=stage_s.at[pl.ds((to * 2 + half) * both + first, count)], dst_ref=out_hbm.at[block(half), pl.ds(first, count)],
            send_sem=send_sem.at[to, half, kind], recv_sem=recv_sem.at[chip, half, kind],
            device_id={"sp": to * 2 + core}, device_id_type=MESH)

    def arrived(away, half, kind, count, first):
        source = (chip + chips - away) % chips
        return pltpu.make_async_remote_copy(
            src_ref=stage_s.at[pl.ds(first, count)], dst_ref=out_hbm.at[source * 2 + (core + half) % 2, pl.ds(first, count)],
            send_sem=send_sem.at[source, half, kind], recv_sem=recv_sem.at[source, half, kind],
            device_id={"sp": source * 2 + core}, device_id_type=MESH)

    def keep(half, kind, count, first):
        return pltpu.make_async_copy(stage_s.at[pl.ds((chip * 2 + half) * both + first, count)], out_hbm.at[block(half), pl.ds(first, count)],
                                     own_sem.at[half, kind])

    def post(u):
        t, half = unit(u)

        @pl.when(t == 1)
        def _():
            for away in range(1, chips):
                send(away, half, 0, 2, 0).start()
            keep(half, 0, 2, 0).start()

        away, sub = query(t)

        @pl.when((t >= 2) & (away > 0))
        def _():
            send(away, half, 1 + sub, wide, 2 + sub * wide).start()

        @pl.when((t >= 2) & (away == 0))
        def _():
            keep(half, 1 + sub, wide, 2 + sub * wide).start()

    def make(u):
        t, half = unit(u)

        @pl.when(half == 0)
        def _():
            pltpu.make_async_copy(wq_hbm.at[:, pl.ds(0, tile)], w_s.at[t % DEPTH], w_sem.at[t % DEPTH]).wait()

    def free(u):
        t, half = unit(u)

        @pl.when(half == 1)
        def _():
            fetch(t + DEPTH)

    def product(u):
        t, half = unit(u)
        raw_s[u % 2] = _dot(a_s[pl.ds(pl.multiple_of(half * own, own), own), :], w_s[t % DEPTH])

    def step(u, _):
        make(u)
        free(u - 1)

        @pl.when(u == 2)
        def _():
            for i in range(own // ROWS):
                swap(i).wait_recv()

        turn(u - 1)
        product(u)
        post(u - 1)

    make(jnp.int32(0))
    product(jnp.int32(0))
    lax.fori_loop(1, total, step, None)
    turn(jnp.int32(total - 1))
    post(jnp.int32(total - 1))
    for i in range(own // ROWS):
        swap(i).wait_send()
    for half in range(2):
        for kind in range(1 + per):
            count, first = (wide, 2 + (kind - 1) * wide) if kind else (2, 0)
            keep(half, kind, count, first).wait()
            for away in range(1, chips):
                send(away, half, kind, count, first).wait_send()
                arrived(away, half, kind, count, first).wait_recv()


def project(x, gain, rot, wq, wk, wv, n):
    own, d = x.shape
    heads = wq.shape[1] // HEAD // n
    tile = n // 2 * HEAD
    kinds = 1 + heads * HEAD // tile
    hbm = pl.BlockSpec(memory_space=pltpu.HBM)
    vmem = pl.BlockSpec(memory_space=pltpu.VMEM)
    return pl.pallas_call(
        functools.partial(_project, n, heads),
        out_shape=jax.ShapeDtypeStruct((n, 2 + heads, own, HEAD), jnp.bfloat16),
        in_specs=[hbm, vmem, vmem, hbm, hbm, hbm],
        out_specs=hbm,
        scratch_shapes=[
            pltpu.VMEM((2 * own, d), jnp.bfloat16),
            pltpu.VMEM((DEPTH, d, tile), jnp.bfloat16),
            pltpu.VMEM((n * (2 + heads), own, HEAD), jnp.bfloat16),
            pltpu.VMEM((2, own, tile), jnp.float32),
            pltpu.SemaphoreType.DMA,
            pltpu.SemaphoreType.DMA((DEPTH,)),
            pltpu.SemaphoreType.DMA((own // ROWS,)),
            pltpu.SemaphoreType.DMA((own // ROWS,)),
            pltpu.SemaphoreType.DMA((2, kinds)),
            pltpu.SemaphoreType.DMA((n // 2, 2, kinds)),
            pltpu.SemaphoreType.DMA((n // 2, 2, kinds)),
        ],
        compiler_params=pltpu.CompilerParams(collective_id=0, has_side_effects=True, vmem_limit_bytes=VMEM),
        name="project",
    )(x, gain[None], rot, wq, wk, wv)


def _finish(n, heads, qkv_hbm, x_hbm, wo_hbm, y_hbm, kv_s, vt_s, q_s, top_s, mix_s, gap_s, eye_s, buf_s, acc_s, w_s, p_s, y_s,
            x_sem, kv_sem, q_sem, w_sem, y_sem, send_sem, recv_sem, p_send, p_recv, free_sem):
    me = lax.axis_index("sp")
    chip, core = me // 2, me % 2
    chips, partner = n // 2, me // 2 * 2 + 1 - me % 2
    own = q_s.shape[2]
    width = heads * HEAD
    cols = heads * own
    tile = w_s.shape[2]
    per = wo_hbm.shape[1] // tile
    total = chips * per
    e = HEAD**-0.5 * LOG2E

    get_kv = [pltpu.make_async_copy(qkv_hbm.at[:, i], kv_s.at[i], kv_sem.at[i]) for i in range(2)]

    def whose(s):
        away, half = _away(s, chips)
        return (chip + away) % chips * 2 + half

    def get_q(s):
        return pltpu.make_async_copy(qkv_hbm.at[whose(s), pl.ds(2, heads)], q_s.at[s % 2], q_sem.at[s % 2])

    def columns(t):
        return pl.ds(pl.multiple_of(t % per * tile, tile), tile)

    def get_x(t):
        return pltpu.make_async_copy(x_hbm.at[:, columns(t)], y_s.at[t % 3], x_sem.at[t % 3])

    for copy in get_kv:
        copy.start()
    get_q(jnp.int32(0)).start()
    for t in range(2):
        get_x(jnp.int32(t)).start()

    def fetch(t):
        slot = t % OUT_DEPTH
        rows = ((chip + chips - t // per) % chips * 2 + core) * width
        return pltpu.make_async_copy(wo_hbm.at[pl.ds(pl.multiple_of(rows, width), width), columns(t)], w_s.at[slot], w_sem.at[slot])

    for t in range(OUT_DEPTH - 1):
        fetch(jnp.int32(t)).start()
    barrier = _greet(me, n)

    eye_s[...] = jnp.where(lax.broadcasted_iota(jnp.int32, eye_s.shape, 0) == lax.broadcasted_iota(jnp.int32, eye_s.shape, 1), 1.0, 0.0).astype(jnp.bfloat16)
    gap_s[...] = lax.broadcasted_iota(jnp.int32, gap_s.shape, 1) - lax.broadcasted_iota(jnp.int32, gap_s.shape, 0)
    vt_s[HEAD:, :] = jnp.ones((vt_s.shape[0] - HEAD, n * own), jnp.bfloat16)
    for copy in get_kv:
        copy.wait()
    for j in range(n):
        vt_s[:HEAD, j * own : (j + 1) * own] = _dot(eye_s[:HEAD, :HEAD], kv_s[1, j], 1, 1).astype(jnp.bfloat16)
    pl.semaphore_wait(barrier, n - 1)

    starts = list(range(0, cols, STRIP))

    def block(slot, first, count, level):
        bk = count * own
        k = kv_s[0, pl.ds(first, count)].reshape(bk, HEAD)
        vt = vt_s[:, pl.ds(pl.multiple_of(first * own, own), bk)]
        q = q_s.at[slot]

        def score(at):
            return _dot(k, q[at // own : (at + STRIP) // own].reshape(STRIP, HEAD), 1, 1)

        def weigh(at, s):
            here = slice(at, at + STRIP)
            if level is not None:
                ok = gap_s[:bk, :] >= -level
                s = jnp.where(jnp.concatenate([ok] * (STRIP // own), 1), s, HIDDEN)
            old = top_s[:, here]
            top = jnp.maximum(old, s.max(axis=0, keepdims=True))
            top_s[:, here] = top
            return jnp.exp2((s - top) * e).astype(jnp.bfloat16), jnp.exp2((old - top) * e)

        def mix(at, p, keep):
            here = slice(at, at + STRIP)
            mix_s[:, here] = mix_s[:, here] * keep + _dot(vt, p)

        s_next, before = score(starts[0]), None
        for i, at in enumerate(starts):
            s = s_next
            if i + 1 < len(starts):
                s_next = score(starts[i + 1])
            p, keep = weigh(at, s)
            if before is not None:
                mix(*before)
            before = (at, p, keep)
        mix(*before)

    def send(s):
        away, half = _away(s, chips)
        return pltpu.make_async_remote_copy(
            src_ref=buf_s.at[n + s], dst_ref=buf_s.at[chip * 2 + half], send_sem=send_sem.at[s], recv_sem=recv_sem.at[chip, half],
            device_id={"sp": (chip + away) % chips * 2 + core}, device_id_type=MESH)

    def attend(s, _):
        b = whose(s)
        slot = s % 2
        get_q(s).wait()

        @pl.when(s + 1 < n)
        def _():
            get_q(s + 1).start()

        top_s[...] = jnp.full(top_s.shape, NEG, jnp.float32)
        mix_s[...] = jnp.zeros(mix_s.shape, jnp.float32)
        lax.fori_loop(0, b // 2, lambda j, _: block(slot, 2 * j, 2, None), None)

        @pl.when(b % 2 == 0)
        def _():
            block(slot, b, 1, 0)

        @pl.when(b % 2 == 1)
        def _():
            block(slot, b - 1, 2, own)

        mine = s // (n - 2)
        to = (n + s) * (1 - mine) + b * mine
        for h in range(heads):
            here = slice(h * own, (h + 1) * own)
            done = (mix_s[:HEAD, here] * (1 / mix_s[HEAD : HEAD + 1, here])).astype(jnp.bfloat16)
            buf_s[to, :, h * HEAD : (h + 1) * HEAD] = _dot(eye_s[...], done, 1, 1).astype(jnp.bfloat16)

        @pl.when(s < n - 2)
        def _():
            send(s).start()

    lax.fori_loop(0, n, attend, None)

    def put(t):
        return pltpu.make_async_copy(y_s.at[t % 3], y_hbm.at[:, columns(t)], y_sem.at[t % 3])

    def give(t):
        return pltpu.make_async_remote_copy(
            src_ref=acc_s.at[1 - core, :, columns(t)], dst_ref=p_s.at[t % SLOTS], send_sem=p_send.at[t], recv_sem=p_recv.at[t % SLOTS],
            device_id={"sp": partner}, device_id_type=MESH)

    def close(t):
        get_x(t).wait()
        give(t).wait_recv()
        y_s[t % 3] = (y_s[t % 3].astype(jnp.float32) + (acc_s[core, :, columns(t)] + p_s[t % SLOTS])).astype(jnp.bfloat16)
        put(t).start()

        @pl.when(t + SLOTS < per)
        def _():
            pl.semaphore_signal(free_sem, inc=1, device_id={"sp": partner}, device_id_type=MESH)

        @pl.when(t > 0)
        def _():
            put(t - 1).wait()

        @pl.when(t + 2 < per)
        def _():
            get_x(t + 2).start()

    def step(t, _, first=False):
        slot = t % OUT_DEPTH
        turn = t // per
        source = (chip + chips - turn) % chips

        if not first:
            @pl.when(t % per == 0)
            def _():
                for half in range(2):
                    pltpu.make_async_remote_copy(
                        src_ref=buf_s.at[n], dst_ref=buf_s.at[source * 2 + half], send_sem=send_sem.at[0], recv_sem=recv_sem.at[source, half],
                        device_id={"sp": source * 2 + core}, device_id_type=MESH).wait_recv()

        fetch(t).wait()

        @pl.when(t + OUT_DEPTH - 1 < total)
        def _():
            fetch(t + OUT_DEPTH - 1).start()

        got = _dot(buf_s[pl.ds(source * 2, 2)].reshape(2 * own, width), w_s[slot]).reshape(2, own, tile)
        if first:
            acc_s[:, :, columns(t)] = got
        else:
            acc_s[:, :, columns(t)] += got

            @pl.when(turn == chips - 1)
            def _():
                c = t - (chips - 1) * per

                @pl.when(c >= SLOTS)
                def _():
                    pl.semaphore_wait(free_sem, 1)

                give(c).start()

                @pl.when(c >= LAG)
                def _():
                    close(c - LAG)

    lax.fori_loop(0, per, functools.partial(step, first=True), None)
    lax.fori_loop(per, total, step, None)
    for t in range(per - LAG, per):
        close(jnp.int32(t))
    put(jnp.int32(per - 1)).wait()
    for t in range(per):
        give(t).wait_send()
    for s in range(n - 2):
        send(s).wait_send()


def finish(qkv, x, wo, n):
    own, d = x.shape
    heads = qkv.shape[1] - 2
    hbm = pl.BlockSpec(memory_space=pltpu.HBM)
    cols = heads * own
    return pl.pallas_call(
        functools.partial(_finish, n, heads),
        out_shape=jax.ShapeDtypeStruct((own, wo.shape[1]), jnp.bfloat16),
        in_specs=[hbm] * 3,
        out_specs=hbm,
        scratch_shapes=[
            pltpu.VMEM((2, n, own, HEAD), jnp.bfloat16),
            pltpu.VMEM((HEAD + 16, n * own), jnp.bfloat16),
            pltpu.VMEM((2, heads, own, HEAD), jnp.bfloat16),
            pltpu.VMEM((1, cols), jnp.float32),
            pltpu.VMEM((HEAD + 16, cols), jnp.float32),
            pltpu.VMEM((2 * own, own), jnp.int32),
            pltpu.VMEM((own, own), jnp.bfloat16),
            pltpu.VMEM((2 * n - 2, own, heads * HEAD), jnp.bfloat16),
            pltpu.VMEM((2, own, wo.shape[1]), jnp.float32),
            pltpu.VMEM((OUT_DEPTH, heads * HEAD, OUT_TILE), jnp.bfloat16),
            pltpu.VMEM((SLOTS, own, OUT_TILE), jnp.float32),
            pltpu.VMEM((3, own, OUT_TILE), jnp.bfloat16),
            pltpu.SemaphoreType.DMA((3,)),
            pltpu.SemaphoreType.DMA((2,)),
            pltpu.SemaphoreType.DMA((2,)),
            pltpu.SemaphoreType.DMA((OUT_DEPTH,)),
            pltpu.SemaphoreType.DMA((3,)),
            pltpu.SemaphoreType.DMA((n - 2,)),
            pltpu.SemaphoreType.DMA((n // 2, 2)),
            pltpu.SemaphoreType.DMA((wo.shape[1] // OUT_TILE,)),
            pltpu.SemaphoreType.DMA((SLOTS,)),
            pltpu.SemaphoreType.REGULAR,
        ],
        compiler_params=pltpu.CompilerParams(collective_id=1, has_side_effects=True, vmem_limit_bytes=VMEM),
        name="finish",
    )(qkv, x, wo)


def solution(mesh):
    n = mesh.shape["sp"]

    def step(x, gain, wq, wk, wv, wo):
        own = x.shape[0]
        me, half = lax.axis_index("sp"), HEAD // 2
        place = (jnp.stack([me, me // 2 * 2 + 1 - me % 2])[:, None] * own + jnp.arange(own)).astype(jnp.float32)
        angle = place[..., None] * THETA ** (-jnp.arange(half, dtype=jnp.float32) / half)
        angle = jnp.concatenate([angle, jnp.zeros_like(angle[:1])])
        cos, sin = jnp.cos(angle), jnp.sin(angle)
        rot = jnp.stack([jnp.concatenate([cos, cos], -1), jnp.concatenate([-sin, sin], -1)], 1)
        qkv = project(x, gain, rot, wq, wk, wv, n)
        return finish(qkv, x, wo, n)

    tokens, whole = P(("dp", "sp"), None), P(None, None)
    return jax.shard_map(
        step,
        mesh=mesh,
        in_specs=(tokens, P(None), whole, whole, whole, whole),
        out_specs=tokens,
        check_vma=False,
    )
```

```python
import functools

import jax
import jax.numpy as jnp
from jax import lax
from jax.experimental import pallas as pl
from jax.experimental.pallas import tpu as pltpu
from jax.sharding import PartitionSpec as P

HEAD = 128
THETA = 10000
NEG = -1e30
HIDDEN = 2 * NEG
LOG2E = 1.4426950408889634
VMEM = 64 * 2**20 - 2**16
MESH = pl.DeviceIdType.MESH

DEPTH = 3
OUT_TILE = 1024
SLOTS = 3
LAG = 2
STRIP = 512
ROWS, CHUNK = 64, 512


def _dot(a, b, ca=1, cb=0):
    return lax.dot_general(a, b, (((ca,), (cb,)), ((), ())), preferred_element_type=jnp.float32)


def _away(s):
    late = s // 4
    return (1 - late) * (3 - 2 * (s % 2)) + late * (2 - (s - 4) // 2 * 2), (1 - late) * (s // 2) + late * (s % 2)


def _greet(me, n):
    barrier = pltpu.get_barrier_semaphore()
    for i in range(1, n):
        pl.semaphore_signal(barrier, inc=1, device_id={"sp": (me + i) % n}, device_id_type=MESH)
    return barrier


def _project(n, heads, x_hbm, gain_ref, rot_ref, wq_hbm, wk_hbm, wv_hbm, out_hbm, a_s, w_s, stage_s, raw_s,
             x_sem, w_sem, a_send, a_recv, own_sem, send_sem, recv_sem):
    me = lax.axis_index("sp")
    chip, core = me // 2, me % 2
    chips, partner = n // 2, me // 2 * 2 + 1 - me % 2
    own, d = x_hbm.shape
    tile = w_s.shape[2]
    wide = tile // HEAD
    per = heads * HEAD // tile
    both = 2 + heads
    tiles = 2 + chips * per

    get_x = [pltpu.make_async_copy(x_hbm.at[pl.ds(i * ROWS, ROWS)], a_s.at[pl.ds(i * ROWS, ROWS)], x_sem.at[i]) for i in range(own // ROWS)]
    for copy in get_x:
        copy.start()

    def query(t):
        j, far = jnp.maximum(t - 2, 0), chips - 1
        last = jnp.minimum(j // (per * far), 1)
        return (j % far + 1) * (1 - last), j // far * (1 - last) + (j - per * far) * last

    def fetch(t):
        slot = t % DEPTH

        def pair(ref):
            for i in range(chips):
                pltpu.make_async_copy(ref.at[:, pl.ds(pl.multiple_of((2 * i + core) * HEAD, HEAD), HEAD)],
                                      w_s.at[slot, :, pl.ds(i * HEAD, HEAD)], w_sem.at[slot]).start()

        @pl.when(t == 0)
        def _():
            pair(wk_hbm)

        @pl.when(t == 1)
        def _():
            pair(wv_hbm)

        @pl.when((t >= 2) & (t < tiles))
        def _():
            away, sub = query(t)
            column = (((chip + away) % chips * 2 + core) * per + sub) * tile
            pltpu.make_async_copy(wq_hbm.at[:, pl.ds(pl.multiple_of(column, tile), tile)], w_s.at[slot], w_sem.at[slot]).start()

    for t in range(DEPTH):
        fetch(jnp.int32(t))
    barrier = _greet(me, n)

    def norm(i):
        rows = pl.ds(pl.multiple_of(i * ROWS, ROWS), ROWS)

        def chunk(c):
            return pl.ds(pl.multiple_of(c * CHUNK, CHUNK), CHUNK)

        def square(c, total):
            w = a_s[rows, chunk(c)].astype(jnp.float32)
            w = w * w
            return total + sum(w[:, k : k + HEAD] for k in range(0, CHUNK, HEAD))

        total = lax.fori_loop(0, d // CHUNK, square, jnp.zeros((ROWS, HEAD), jnp.float32))
        scale = lax.rsqrt(total.sum(-1, keepdims=True) * (1 / d) + 1e-6)

        def apply(c, _):
            w = a_s[rows, chunk(c)].astype(jnp.float32)
            a_s[rows, chunk(c)] = (w * scale * gain_ref[:, chunk(c)].astype(jnp.float32)).astype(jnp.bfloat16)

        lax.fori_loop(0, d // CHUNK, apply, None)

    def swap(i):
        return pltpu.make_async_remote_copy(
            src_ref=a_s.at[pl.ds(i * ROWS, ROWS)], dst_ref=a_s.at[pl.ds(own + i * ROWS, ROWS)], send_sem=a_send.at[i], recv_sem=a_recv.at[i],
            device_id={"sp": partner}, device_id_type=MESH)

    for i in range(own // ROWS):
        get_x[i].wait()
        norm(i)
        if i == 0:
            pl.semaphore_wait(barrier, n - 1)
        swap(i).start()

    def block(half):
        return chip * 2 + (core + half) % 2

    def turn(t, half):
        away, sub = query(t)
        q = jnp.minimum(t // 2, 1)
        base = q * (((chip + away) % chips * 2 + half) * both + 2 + sub * wide) + (1 - q) * (half * both + t)
        gap = q + (1 - q) * 2 * both
        angle = q * half + (1 - q) * (half * (1 - t) + 2 * t)
        for i in range(wide):
            got = raw_s[pl.ds(pl.multiple_of(half * own, own), own), i * HEAD : (i + 1) * HEAD].astype(jnp.bfloat16).astype(jnp.float32)
            got = got * rot_ref[angle, 0] + pltpu.roll(got, HEAD // 2, 1) * rot_ref[angle, 1]
            stage_s[base + i * gap] = got.astype(jnp.bfloat16)

    def send(away, half, kind, count, first):
        to = (chip + away) % chips
        return pltpu.make_async_remote_copy(
            src_ref=stage_s.at[pl.ds((to * 2 + half) * both + first, count)], dst_ref=out_hbm.at[block(half), pl.ds(first, count)],
            send_sem=send_sem.at[to, half, kind], recv_sem=recv_sem.at[chip, half, kind],
            device_id={"sp": to * 2 + core}, device_id_type=MESH)

    def arrived(away, half, kind, count, first):
        source = (chip + chips - away) % chips
        return pltpu.make_async_remote_copy(
            src_ref=stage_s.at[pl.ds(first, count)], dst_ref=out_hbm.at[source * 2 + (core + half) % 2, pl.ds(first, count)],
            send_sem=send_sem.at[source, half, kind], recv_sem=recv_sem.at[source, half, kind],
            device_id={"sp": source * 2 + core}, device_id_type=MESH)

    def keep(half, kind, count, first):
        return pltpu.make_async_copy(stage_s.at[pl.ds((chip * 2 + half) * both + first, count)], out_hbm.at[block(half), pl.ds(first, count)],
                                     own_sem.at[half, kind])

    def post(t, half):
        @pl.when(t == 1)
        def _():
            for away in range(1, chips):
                send(away, half, 0, 2, 0).start()
            keep(half, 0, 2, 0).start()

        away, sub = query(t)

        @pl.when((t >= 2) & (away > 0))
        def _():
            send(away, half, 1 + sub, wide, 2 + sub * wide).start()

        @pl.when((t >= 2) & (away == 0))
        def _():
            keep(half, 1 + sub, wide, 2 + sub * wide).start()

    def ready(t):
        pltpu.make_async_copy(wq_hbm.at[:, pl.ds(0, tile)], w_s.at[t % DEPTH], w_sem.at[t % DEPTH]).wait()

    def early(u, _):
        t, half = u % 2, u // 2

        @pl.when(half == 0)
        def _():
            ready(t)

        @pl.when(u == 2)
        def _():
            for i in range(own // ROWS):
                swap(i).wait_recv()

        rows = pl.ds(pl.multiple_of(half * own, own), own)
        raw_s[rows, :] = _dot(a_s[rows, :], w_s[t])
        turn(t, half)
        post(t, half)

        @pl.when(half == 1)
        def _():
            fetch(t + DEPTH)

    def step(t, _):
        ready(t)
        raw_s[...] = _dot(a_s[...], w_s[t % DEPTH])
        fetch(t + DEPTH)
        for half in range(2):
            turn(t, half)
            post(t, half)

    lax.fori_loop(0, 4, early, None)
    lax.fori_loop(2, tiles, step, None)
    for i in range(own // ROWS):
        swap(i).wait_send()
    for half in range(2):
        for kind in range(1 + per):
            count, first = (wide, 2 + (kind - 1) * wide) if kind else (2, 0)
            keep(half, kind, count, first).wait()
            for away in range(1, chips):
                send(away, half, kind, count, first).wait_send()
                arrived(away, half, kind, count, first).wait_recv()


def project(x, gain, rot, wq, wk, wv, n):
    own, d = x.shape
    heads = wq.shape[1] // HEAD // n
    tile = n // 2 * HEAD
    kinds = 1 + heads * HEAD // tile
    hbm = pl.BlockSpec(memory_space=pltpu.HBM)
    vmem = pl.BlockSpec(memory_space=pltpu.VMEM)
    return pl.pallas_call(
        functools.partial(_project, n, heads),
        out_shape=jax.ShapeDtypeStruct((n, 2 + heads, own, HEAD), jnp.bfloat16),
        in_specs=[hbm, vmem, vmem, hbm, hbm, hbm],
        out_specs=hbm,
        scratch_shapes=[
            pltpu.VMEM((2 * own, d), jnp.bfloat16),
            pltpu.VMEM((DEPTH, d, tile), jnp.bfloat16),
            pltpu.VMEM((n * (2 + heads), own, HEAD), jnp.bfloat16),
            pltpu.VMEM((2 * own, tile), jnp.float32),
            pltpu.SemaphoreType.DMA((own // ROWS,)),
            pltpu.SemaphoreType.DMA((DEPTH,)),
            pltpu.SemaphoreType.DMA((own // ROWS,)),
            pltpu.SemaphoreType.DMA((own // ROWS,)),
            pltpu.SemaphoreType.DMA((2, kinds)),
            pltpu.SemaphoreType.DMA((n // 2, 2, kinds)),
            pltpu.SemaphoreType.DMA((n // 2, 2, kinds)),
        ],
        compiler_params=pltpu.CompilerParams(collective_id=0, has_side_effects=True, vmem_limit_bytes=VMEM),
        name="project",
    )(x, gain[None], rot, wq, wk, wv)


def _finish(n, heads, qkv_hbm, x_hbm, wo_hbm, y_hbm, kv_s, vt_s, q_s, top_s, mix_s, gap_s, eye_s, buf_s, got_s, acc_s, w_s, p_s, y_s,
            x_sem, kv_sem, q_sem, w_sem, y_sem, send_sem, recv_sem, p_send, p_recv, free_sem):
    me = lax.axis_index("sp")
    chip, core = me // 2, me % 2
    chips, partner = n // 2, me // 2 * 2 + 1 - me % 2
    own = q_s.shape[2]
    width = heads * HEAD
    cols = heads * own
    tile = w_s.shape[2]
    per = wo_hbm.shape[1] // tile
    e = HEAD**-0.5 * LOG2E

    get_kv = [pltpu.make_async_copy(qkv_hbm.at[:, i], kv_s.at[i], kv_sem.at[i]) for i in range(2)]

    swap = chip // (chips - 1)
    turns = ((0,), (3 - 2 * swap,), (1 + 2 * swap, 2))

    def whose(s):
        away, half = _away(s)
        return (chip + away) % chips * 2 + half

    def get_q(s):
        return pltpu.make_async_copy(qkv_hbm.at[whose(s), pl.ds(2, heads)], q_s.at[s % 2], q_sem.at[s % 2])

    def columns(t):
        return pl.ds(pl.multiple_of(t % per * tile, tile), tile)

    def get_x(t):
        return pltpu.make_async_copy(x_hbm.at[:, columns(t)], y_s.at[t % 3], x_sem.at[t % 3])

    for copy in get_kv:
        copy.start()
    get_q(jnp.int32(0)).start()
    for t in range(2):
        get_x(jnp.int32(t)).start()

    def fetch(turn, c):
        slot = (turn * per + c) % 2
        for i, away in enumerate(turns[turn]):
            rows = ((chip + chips - away) % chips * 2 + core) * width
            pltpu.make_async_copy(wo_hbm.at[pl.ds(pl.multiple_of(rows, width), width), columns(c)], w_s.at[slot, pl.ds(i * width, width)],
                                  w_sem.at[slot]).start()

    fetch(0, jnp.int32(0))
    barrier = _greet(me, n)

    eye_s[...] = jnp.where(lax.broadcasted_iota(jnp.int32, eye_s.shape, 0) == lax.broadcasted_iota(jnp.int32, eye_s.shape, 1), 1.0, 0.0).astype(jnp.bfloat16)
    gap_s[...] = lax.broadcasted_iota(jnp.int32, gap_s.shape, 1) - lax.broadcasted_iota(jnp.int32, gap_s.shape, 0)
    vt_s[HEAD:, :] = jnp.ones((vt_s.shape[0] - HEAD, n * own), jnp.bfloat16)
    for copy in get_kv:
        copy.wait()
    for j in range(n):
        vt_s[:HEAD, j * own : (j + 1) * own] = _dot(eye_s[:HEAD, :HEAD], kv_s[1, j], 1, 1).astype(jnp.bfloat16)
    pl.semaphore_wait(barrier, n - 1)

    starts = list(range(0, cols, STRIP))

    def block(slot, first, count, level):
        bk = count * own
        k = kv_s[0, pl.ds(first, count)].reshape(bk, HEAD)
        vt = vt_s[:, pl.ds(pl.multiple_of(first * own, own), bk)]
        q = q_s.at[slot]

        def score(at):
            return _dot(k, q[at // own : (at + STRIP) // own].reshape(STRIP, HEAD), 1, 1)

        def weigh(at, s):
            here = slice(at, at + STRIP)
            if level is not None:
                ok = gap_s[...] >= 0
                cut = jnp.where(jnp.concatenate([ok] * (STRIP // own), 1), s[level:], HIDDEN)
                s = jnp.concatenate([s[:level], cut], 0) if level else cut
            old = top_s[:, here]
            top = jnp.maximum(old, s.max(axis=0, keepdims=True))
            top_s[:, here] = top
            return jnp.exp2((s - top) * e).astype(jnp.bfloat16), jnp.exp2((old - top) * e)

        def mix(at, p, keep):
            here = slice(at, at + STRIP)
            mix_s[:, here] = mix_s[:, here] * keep + _dot(vt, p)

        s_next, before = score(starts[0]), None
        for i, at in enumerate(starts):
            s = s_next
            if i + 1 < len(starts):
                s_next = score(starts[i + 1])
            p, keep = weigh(at, s)
            if before is not None:
                mix(*before)
            before = (at, p, keep)
        mix(*before)

    def seat(to, away, half):
        late, odd = to // (chips - 1), away % 2
        at = odd * (1 + late + (3 - away) // 2 * (1 - 2 * late)) + (1 - odd) * (away // 2 * 3)
        return got_s.at[at // 2, half, :, pl.ds(pl.multiple_of(at % 2 * width, width), width)]

    def send(s):
        away, half = _away(s)
        return pltpu.make_async_remote_copy(
            src_ref=buf_s.at[s], dst_ref=seat((chip + away) % chips, away, half), send_sem=send_sem.at[s], recv_sem=recv_sem.at[away, half],
            device_id={"sp": (chip + away) % chips * 2 + core}, device_id_type=MESH)

    def attend(s, _):
        b = whose(s)
        slot = s % 2
        get_q(s).wait()

        @pl.when(s + 1 < n)
        def _():
            get_q(s + 1).start()

        top_s[...] = jnp.full(top_s.shape, NEG, jnp.float32)
        mix_s[...] = jnp.zeros(mix_s.shape, jnp.float32)
        lax.fori_loop(0, b // 2, lambda j, _: block(slot, 2 * j, 2, None), None)

        @pl.when(b % 2 == 0)
        def _():
            block(slot, b, 1, 0)

        @pl.when(b % 2 == 1)
        def _():
            block(slot, b - 1, 2, own)

        def result(h):
            done = [(mix_s[:HEAD, g * own : (g + 1) * own] * (1 / mix_s[HEAD : HEAD + 1, g * own : (g + 1) * own])).astype(jnp.bfloat16) for g in (h, h + 1)]
            return _dot(eye_s[...], jnp.concatenate(done, 0), 1, 1).astype(jnp.bfloat16)

        @pl.when(s < n - 2)
        def _():
            for h in range(0, heads, 2):
                buf_s[s, :, h * HEAD : (h + 2) * HEAD] = result(h)

        @pl.when(s >= n - 2)
        def _():
            for h in range(0, heads, 2):
                got_s[0, s - (n - 2), :, h * HEAD : (h + 2) * HEAD] = result(h)

        @pl.when(s < n - 2)
        def _():
            send(s).start()

    lax.fori_loop(0, n, attend, None)

    def put(t):
        return pltpu.make_async_copy(y_s.at[t % 3], y_hbm.at[:, columns(t)], y_sem.at[t % 3])

    def give(t):
        return pltpu.make_async_remote_copy(
            src_ref=acc_s.at[1 - core, :, columns(t)], dst_ref=p_s.at[t % SLOTS], send_sem=p_send.at[t], recv_sem=p_recv.at[t % SLOTS],
            device_id={"sp": partner}, device_id_type=MESH)

    def close(t):
        get_x(t).wait()
        give(t).wait_recv()
        y_s[t % 3] = (y_s[t % 3].astype(jnp.float32) + (acc_s[core, :, columns(t)] + p_s[t % SLOTS])).astype(jnp.bfloat16)
        put(t).start()

        @pl.when(t + SLOTS < per)
        def _():
            pl.semaphore_signal(free_sem, inc=1, device_id={"sp": partner}, device_id_type=MESH)

        @pl.when(t > 0)
        def _():
            put(t - 1).wait()

        @pl.when(t + 2 < per)
        def _():
            get_x(t + 2).start()

    def step(c, _, turn):
        near = turns[turn]
        slot = (turn * per + c) % 2
        deep = len(near) * width

        @pl.when(c == 0)
        def _():
            for away in near:
                for half in range(2 if turn else 0):
                    pltpu.make_async_remote_copy(
                        src_ref=buf_s.at[0], dst_ref=seat(chip, away, half), send_sem=send_sem.at[0], recv_sem=recv_sem.at[away, half],
                        device_id={"sp": (chip + chips - away) % chips * 2 + core}, device_id_type=MESH).wait_recv()

        pltpu.make_async_copy(wo_hbm.at[pl.ds(0, deep), columns(c)], w_s.at[slot, pl.ds(0, deep)], w_sem.at[slot]).wait()

        @pl.when(c + 1 < per)
        def _():
            fetch(turn, c + 1)

        if turn + 1 < len(turns):
            @pl.when(c + 1 == per)
            def _():
                fetch(turn + 1, jnp.int32(0))

        at = turn
        left = got_s[at // 2, :, :, at % 2 * width : at % 2 * width + deep].reshape(2 * own, deep)
        got = _dot(left, w_s[slot, :deep]).reshape(2, own, tile)
        if turn == 0:
            acc_s[:, :, columns(c)] = got
        else:
            acc_s[:, :, columns(c)] += got
        if turn == len(turns) - 1:
            @pl.when(c >= SLOTS)
            def _():
                pl.semaphore_wait(free_sem, 1)

            give(c).start()

            @pl.when(c >= LAG)
            def _():
                close(c - LAG)

    for turn in range(len(turns)):
        lax.fori_loop(0, per, functools.partial(step, turn=turn), None)
    for t in range(per - LAG, per):
        close(jnp.int32(t))
    put(jnp.int32(per - 1)).wait()
    for t in range(per):
        give(t).wait_send()
    for s in range(n - 2):
        send(s).wait_send()


def finish(qkv, x, wo, n):
    own, d = x.shape
    heads = qkv.shape[1] - 2
    hbm = pl.BlockSpec(memory_space=pltpu.HBM)
    cols = heads * own
    return pl.pallas_call(
        functools.partial(_finish, n, heads),
        out_shape=jax.ShapeDtypeStruct((own, wo.shape[1]), jnp.bfloat16),
        in_specs=[hbm] * 3,
        out_specs=hbm,
        scratch_shapes=[
            pltpu.VMEM((2, n, own, HEAD), jnp.bfloat16),
            pltpu.VMEM((HEAD + 16, n * own), jnp.bfloat16),
            pltpu.VMEM((2, heads, own, HEAD), jnp.bfloat16),
            pltpu.VMEM((1, cols), jnp.float32),
            pltpu.VMEM((HEAD + 16, cols), jnp.float32),
            pltpu.VMEM((own, own), jnp.int32),
            pltpu.VMEM((own, own), jnp.bfloat16),
            pltpu.VMEM((n - 2, own, heads * HEAD), jnp.bfloat16),
            pltpu.VMEM((n // 4, 2, own, 2 * heads * HEAD), jnp.bfloat16),
            pltpu.VMEM((2, own, wo.shape[1]), jnp.float32),
            pltpu.VMEM((2, 2 * heads * HEAD, OUT_TILE), jnp.bfloat16),
            pltpu.VMEM((SLOTS, own, OUT_TILE), jnp.float32),
            pltpu.VMEM((3, own, OUT_TILE), jnp.bfloat16),
            pltpu.SemaphoreType.DMA((3,)),
            pltpu.SemaphoreType.DMA((2,)),
            pltpu.SemaphoreType.DMA((2,)),
            pltpu.SemaphoreType.DMA((2,)),
            pltpu.SemaphoreType.DMA((3,)),
            pltpu.SemaphoreType.DMA((n - 2,)),
            pltpu.SemaphoreType.DMA((n // 2, 2)),
            pltpu.SemaphoreType.DMA((wo.shape[1] // OUT_TILE,)),
            pltpu.SemaphoreType.DMA((SLOTS,)),
            pltpu.SemaphoreType.REGULAR,
        ],
        compiler_params=pltpu.CompilerParams(collective_id=1, has_side_effects=True, vmem_limit_bytes=VMEM),
        name="finish",
    )(qkv, x, wo)


def solution(mesh):
    n = mesh.shape["sp"]

    def step(x, gain, wq, wk, wv, wo):
        own = x.shape[0]
        me, half = lax.axis_index("sp"), HEAD // 2
        place = (jnp.stack([me, me // 2 * 2 + 1 - me % 2])[:, None] * own + jnp.arange(own)).astype(jnp.float32)
        angle = place[..., None] * THETA ** (-jnp.arange(half, dtype=jnp.float32) / half)
        angle = jnp.concatenate([angle, jnp.zeros_like(angle[:1])])
        cos, sin = jnp.cos(angle), jnp.sin(angle)
        rot = jnp.stack([jnp.concatenate([cos, cos], -1), jnp.concatenate([-sin, sin], -1)], 1)
        qkv = project(x, gain, rot, wq, wk, wv, n)
        return finish(qkv, x, wo, n)

    tokens, whole = P(("dp", "sp"), None), P(None, None)
    return jax.shard_map(
        step,
        mesh=mesh,
        in_specs=(tokens, P(None), whole, whole, whole, whole),
        out_specs=tokens,
        check_vma=False,
    )
```
